256 devices in a mesh: grp: 16 (over y, x), ep: 16 (over z, core).
Axes of the slice: x: 4, y: 4, z: 8, core: 2. Of those that a mesh axis runs over, the one named last changes fastest.
Arguments:
- tokens: bfloat16 [24576, 4096], P(('grp', 'ep')), may hold values from -6 to 6
- hash_expert: int32 [24576, 1], P(('grp', 'ep')), may hold values from 0 to 15, as said below
- gate_weight: bfloat16 [16, 4096, 4096], P('ep', None, 'grp'), may hold values from -0.09375 to 0.09375
- up_weight: bfloat16 [16, 4096, 4096], P('ep', None, 'grp'), may hold values from -0.09375 to 0.09375
- down_weight: bfloat16 [16, 4096, 4096], P('ep', 'grp'), may hold values from -0.09375 to 0.09375
Outputs:
- combined: bfloat16 [24576, 4096], P(('grp', 'ep'))
- expert_load: float32 [16], replicated
- balance: float32 [], replicated
The draws below stay inside these ranges and needn't reach their ends.
Inputs may be any that keep to these rules, and one draw needn't show every extreme that they name: `hash_expert`: among the 96 rows of one device no expert is named more than 9 times; on every device some expert is named exactly 9 times; every expert is named by some row.
All inputs are finite; a program needn't handle non-finite values.
Results may differ from the reference program's by a relative error of at most 0.014.
Values may be sent and summed in bfloat16 or wider, within the bound.
A program may use at most 128 MiB of HBM per device.

```python
import jax
import jax.numpy as jnp
from jax import lax

D = 4096
FF = 4096
TOK_DEV = 96
EXPERT_COUNT = 16
CAP = 9
TOKENS = 24576
N_GRP = 16


def draw_hash_expert(key, part):
    device_count = TOKENS // TOK_DEV
    tickets = EXPERT_COUNT * CAP
    base_key = jax.random.fold_in(key, 17)
    rank_key, devices_key = jax.random.split(base_key, 2)
    expert_demand = jax.random.permutation(rank_key, EXPERT_COUNT).astype(jnp.int32)
    extra_credit = expert_demand * 1024 // EXPERT_COUNT
    voucher_expert = (jnp.arange(tickets, dtype=jnp.int32) // CAP).astype(jnp.int32)
    voucher_credit = jnp.take(extra_credit, voucher_expert)
    forced_expert = (jnp.arange(device_count, dtype=jnp.int32) * EXPERT_COUNT // device_count).astype(jnp.int32)

    def one_device(device_key, pinned_choice):
        noise_key, order_key = jax.random.split(device_key, 2)
        random_jitter = jax.random.randint(noise_key, (tickets,), 0, 1024, dtype=jnp.int32)
        routing_score = random_jitter + voucher_credit + jnp.where(voucher_expert == pinned_choice, 4096, 0).astype(jnp.int32)
        routing_score = routing_score * tickets + jnp.arange(tickets, dtype=jnp.int32)
        ranking = jnp.argsort(-routing_score, stable=True)
        chosen = ranking[:TOK_DEV]
        named = jnp.take(voucher_expert, chosen)
        return jax.random.permutation(order_key, named).astype(jnp.int32)
    device_keys = jax.random.split(devices_key, device_count)
    named = jax.vmap(one_device)(device_keys, forced_expert)
    return named.astype(jnp.int32).reshape(TOKENS, 1)


def block_scale(stream_key, dims, cuts, least, largest):
    gain, own = 1.0, jax.random.fold_in(stream_key, 6)
    for position, blocks in cuts:
        heights = jnp.exp(jax.random.uniform(jax.random.fold_in(own, position), (blocks,), jnp.float32, least / len(cuts), largest / len(cuts)))
        gain = gain * jnp.repeat(heights, dims[position] // blocks).reshape([-1 if axis == position else 1 for axis in range(len(dims))])
    return gain


def bell_draw(rng, shape, scale, most, cuts=(), held_as=jnp.bfloat16):
    loudness = block_scale(rng, shape, cuts, -0.22, 0.18) if cuts else 1.0
    entries = jax.random.normal(rng, shape, jnp.float32) * scale * loudness
    return jnp.minimum(jnp.maximum(entries, -most), most).astype(held_as)


def setup_inputs(seed: int = 0) -> dict:
    key_of = jax.random.split(jax.random.key(seed), 6)
    tokens = bell_draw(key_of[0], (TOKENS, D), 1.0, 6.0, ((0, 256),))
    hash_expert = draw_hash_expert(jax.random.fold_in(key_of[5], 71), 0)
    gate_weight = bell_draw(key_of[2], (EXPERT_COUNT, D, FF), D ** -0.5, 0.09375, ((0, 16), (2, 16)))
    up_weight = bell_draw(key_of[3], (EXPERT_COUNT, D, FF), D ** -0.5, 0.09375, ((0, 16), (2, 16)))
    down_weight = bell_draw(key_of[4], (EXPERT_COUNT, FF, D), FF ** -0.5, 0.09375, ((0, 16), (1, 16)))
    return dict(tokens=tokens, hash_expert=hash_expert, gate_weight=gate_weight, up_weight=up_weight, down_weight=down_weight)


eps = 1e-06

def reference(tokens, hash_expert, gate_weight, up_weight, down_weight):
    device_count = TOKENS // TOK_DEV
    raw_values = tokens.astype(jnp.float32)
    normed = (raw_values * lax.rsqrt(lax.optimization_barrier(jnp.mean(raw_values * raw_values, axis=-1, keepdims=True)) + eps)).astype(jnp.bfloat16)
    expert = hash_expert[:, 0].reshape(device_count, TOK_DEV)
    onehot = (expert[:, :, None] == jnp.arange(EXPERT_COUNT, dtype=jnp.int32)[None, None, :]).astype(jnp.int32)
    slot_index = lax.optimization_barrier(jnp.sum((jnp.cumsum(onehot, axis=1) - 1) * onehot, axis=-1)).astype(jnp.int32)
    device = jnp.arange(device_count, dtype=jnp.int32)[:, None]
    column = (device * CAP + slot_index).reshape(-1).astype(jnp.int32)
    flat_expert = expert.reshape(-1).astype(jnp.int32)
    buffer = jnp.zeros((EXPERT_COUNT, device_count * CAP, D), jnp.bfloat16).at[flat_expert, column].set(normed)
    slice_width = FF // N_GRP

    def one_expert(operands):
        expert_rows, gate_matrix, up_matrix, down_matrix = operands
        gate_out = jnp.dot(expert_rows, gate_matrix, preferred_element_type=jnp.float32)
        up_out = jnp.dot(expert_rows, up_matrix, preferred_element_type=jnp.float32)
        hidden = (jax.nn.silu(gate_out) * up_out).astype(jnp.bfloat16)

        def add_slice(running, slice_index):
            hidden_part = lax.dynamic_slice_in_dim(hidden, slice_index * slice_width, slice_width, 1)
            down_part = lax.dynamic_slice_in_dim(down_matrix, slice_index * slice_width, slice_width, 0)
            partial_value = jnp.dot(hidden_part, down_part, preferred_element_type=jnp.float32).astype(jnp.bfloat16)
            partial_value = lax.optimization_barrier(partial_value)
            return (running + partial_value.astype(jnp.float32), None)
        running, unused = lax.scan(add_slice, jnp.zeros((expert_rows.shape[0], D), jnp.float32), jnp.arange(N_GRP, dtype=jnp.int32))
        return running.astype(jnp.bfloat16)
    result = lax.map(one_expert, (buffer, gate_weight, up_weight, down_weight))
    combined = result[flat_expert, column]
    counts = lax.optimization_barrier(jnp.sum(onehot.astype(jnp.float32), axis=(0, 1)))
    expert_load = counts * EXPERT_COUNT / TOKENS
    balance = jnp.sum(expert_load * expert_load) / EXPERT_COUNT
    return (combined, expert_load, balance)
```

```python
import functools

import jax
import jax.numpy as jnp
from jax import lax
from jax.experimental import pallas as pl
from jax.experimental.pallas import tpu as pltpu
from jax.sharding import Mesh
from jax.sharding import PartitionSpec as P

EP = ("ep_0", "ep_1")
GRP = ("grp_0", "grp_1")
GRP_EP = ("grp_0", "grp_1", "ep_0", "ep_1")
MESH = pl.DeviceIdType.MESH
CHUNKS = 4

eps = 1e-06


def dot(a, b):
    return jnp.dot(a, b, preferred_element_type=jnp.float32)


def exchange_kernel(
    n_ep,
    packed,
    counts,
    squeeze,
    spread,
    gate,
    up,
    down,
    out,
    totals,
    arrived,
    rows,
    w_in,
    w_out,
    acc,
    hidden,
    far,
    far_in,
    near,
    half_up,
    half_down,
    full_up,
    full_down,
    back,
    count_x,
    count_y,
    count_e,
    z_send,
    z_recv,
    b_send,
    b_recv,
    link_send,
    link_recv,
    w_send,
    w_recv,
    w_local,
    c_send,
    c_recv,
):
    pad, width = packed.shape[1], packed.shape[2]
    own = rows.shape[2]
    units = gate.shape[1]
    cols = width // CHUNKS
    half = cols // 2
    tile = min(256, cols)
    y = lax.axis_index("grp_0")
    x = lax.axis_index("grp_1")
    z = lax.axis_index("ep_0")
    core = lax.axis_index("ep_1")
    me = z * 2 + core
    flip = x + 1 - 2 * (x % 2)
    mirror = 3 - x
    row_mate = mirror + core * (flip - mirror)
    weight_mate = flip + core * (mirror - flip)
    to_rows = {"grp_1": row_mate}
    to_weights = {"grp_1": weight_mate}
    to_up = {"grp_0": (y + 1) % 4}
    to_down = {"grp_0": (y + 3) % 4}

    def ep_peer(d):
        t = (me + d) % n_ep
        return {"ep_0": t // 2, "ep_1": t % 2}

    barrier = pltpu.get_barrier_semaphore()

    def greet(d, carry):
        pl.semaphore_signal(barrier, inc=1, device_id=ep_peer(d), device_id_type=MESH)
        return carry

    lax.fori_loop(1, n_ep, greet, 0)
    for j in range(1, 4):
        pl.semaphore_signal(barrier, inc=1, device_id={"grp_1": (x + j) % 4}, device_id_type=MESH)
        pl.semaphore_signal(barrier, inc=1, device_id={"grp_0": (y + j) % 4}, device_id_type=MESH)
    for r in range(2):
        for c in range(CHUNKS):
            span = pl.ds(c * cols, cols)
            pltpu.make_async_copy(
                (gate, up)[r].at[span, :],
                w_in.at[span, pl.ds(r * units, units)],
                w_local.at[r * CHUNKS + c],
            ).start()
    pltpu.make_async_copy(down, w_out.at[pl.ds(0, units), :], w_local.at[2 * CHUNKS]).start()
    arrived[0] = packed[0]
    count_x[0] = counts[...]
    pl.semaphore_wait(barrier, n_ep - 1 + 6)

    def remote(src, dst, send, recv, device):
        return pltpu.make_async_remote_copy(
            src_ref=src,
            dst_ref=dst,
            send_sem=send,
            recv_sem=recv,
            device_id=device,
            device_id_type=MESH,
        )

    def span_of(c):
        return pl.ds(c * cols, cols)

    def z_copy(c, d, n=None):
        at = d if n is None else pl.ds(d, n)
        return remote(
            packed.at[at, :, span_of(c)],
            arrived.at[at, :, span_of(c)],
            z_send.at[c],
            z_recv.at[c],
            ep_peer(d),
        )

    def back_copy(c, d, n=None):
        at = d if n is None else pl.ds(d, n)
        return remote(
            back.at[at, :, span_of(c)],
            out.at[at, :, span_of(c)],
            b_send.at[c],
            b_recv.at[c],
            ep_peer(n_ep - d),
        )

    def start_all(copy_of, c):
        def go(d, carry):
            copy_of(c, d).start()
            return carry

        lax.fori_loop(1, n_ep, go, 0)

    for c in range(CHUNKS):
        start_all(z_copy, c)

    def weight_copies(c):
        return [
            remote(
                (gate, up)[r].at[span_of(c), :],
                w_in.at[span_of(c), pl.ds((2 + r) * units, units)],
                w_send.at[r * CHUNKS + c],
                w_recv.at[r * CHUNKS + c],
                to_weights,
            )
            for r in range(2)
        ]

    down_copy = remote(
        down,
        w_out.at[pl.ds(units, units), :],
        w_send.at[2 * CHUNKS],
        w_recv.at[2 * CHUNKS],
        to_weights,
    )
    for c in range(CHUNKS):
        for copy in weight_copies(c):
            copy.start()
    down_copy.start()

    def count_copies(buffer, axis, at, sem):
        return [
            remote(buffer.at[0], buffer.at[j], c_send.at[sem], c_recv.at[sem], {axis: (at + j) % 4})
            for j in range(1, 4)
        ]

    def count_all(buffer, n, sem, device):
        return remote(
            buffer.at[pl.ds(1, n)], buffer.at[pl.ds(1, n)], c_send.at[sem], c_recv.at[sem], device
        )

    for copy in count_copies(count_x, "grp_1", x, 0):
        copy.start()

    def link(kind, c, src, dst, device):
        return remote(
            src, dst, link_send.at[kind * CHUNKS + c], link_recv.at[kind * CHUNKS + c], device
        )

    def block(r, k, c):
        return rows.at[r, k, :, span_of(c)]

    def swap_x(c):
        return link(0, c, block(0, 0, c), block(0, 1, c), to_rows)

    def own_up(k, c):
        return link(1 + k, c, block(0, k, c), block(3, k, c), to_up)

    def own_down(k, c):
        return link(3 + k, c, block(0, k, c), block(1, k, c), to_down)

    def pass_up(c):
        return link(5, c, block(3, 0, c), block(2, 0, c), to_up)

    def pass_down(c):
        return link(6, c, block(1, 1, c), block(2, 1, c), to_down)

    def far_copy(c):
        return link(7, c, far.at[:, :, span_of(c)], far_in.at[:, :, span_of(c)], to_rows)

    def half_up_copy(c):
        return link(
            8,
            c,
            near.at[2, :, pl.ds(c * cols, half)],
            half_up.at[:, pl.ds(c * half, half)],
            to_up,
        )

    def half_down_copy(c):
        return link(
            9,
            c,
            near.at[2, :, pl.ds(c * cols + half, half)],
            half_down.at[:, pl.ds(c * half, half)],
            to_down,
        )

    def full_up_copy(c):
        return link(10, c, near.at[1, :, span_of(c)], full_up.at[:, span_of(c)], to_up)

    def full_down_copy(c):
        return link(11, c, near.at[3, :, span_of(c)], full_down.at[:, span_of(c)], to_down)

    def stage_a(c):
        z_copy(c, 1, n_ep - 1).wait_recv()
        span = span_of(c)
        step = min(512, cols)
        for s in range(cols // step):
            part = pl.ds(c * cols + s * step, step)
            rows[0, 0, :, part] = dot(
                squeeze[...], arrived[:, :, part].reshape(n_ep * pad, step)
            ).astype(jnp.bfloat16)
        swap_x(c).start()
        own_up(0, c).start()
        own_down(0, c).start()

    def stage_b(c):
        swap_x(c).wait_recv()
        own_up(1, c).start()
        own_down(1, c).start()

    def stage_c(c):
        own_up(0, c).wait_recv()
        pass_up(c).start()
        own_down(1, c).wait_recv()
        pass_down(c).start()

    def multiply(c, r):
        left = rows[r, :, :, span_of(c)].reshape(2 * own, cols)

        def one(n, carry):
            part = pl.ds(pl.multiple_of(n * units, units), units)
            product = dot(left, w_in[span_of(c), part])
            if c == 0:
                acc[r, :, part] = product
            else:
                acc[r, :, part] += product
            return carry

        lax.fori_loop(0, 4, one, 0)
        if c == CHUNKS - 1:
            for k in range(2):
                g = acc[r, :, pl.ds(2 * k * units, units)]
                u = acc[r, :, pl.ds((2 * k + 1) * units, units)]
                hidden[r, :, pl.ds(k * units, units)] = (jax.nn.silu(g) * u).astype(jnp.bfloat16)

    def stage_d(c):
        for r in range(2):
            pltpu.make_async_copy(
                (gate, up)[r].at[span_of(c), :],
                w_in.at[span_of(c), pl.ds(r * units, units)],
                w_local.at[r * CHUNKS + c],
            ).wait()
        for copy in weight_copies(c):
            copy.wait_recv()
        own_down(0, c).wait_recv()
        own_up(1, c).wait_recv()

        def three(i, carry):
            multiply(c, i + i // 2)
            return carry

        lax.fori_loop(0, 3, three, 0)
        pass_up(c).wait_recv()
        pass_down(c).wait_recv()
        multiply(c, 2)

    def project(c, r, k, s):
        part = pl.ds(pl.multiple_of(c * cols + s * tile, tile), tile)
        return part, dot(hidden[r, pl.ds(k * own, own), :], w_out[:, part])

    def stage_e(c):
        def one(i, carry):
            r, s = i // (cols // tile), i % (cols // tile)
            part, value = project(c, r, 1, s)
            far[r, :, part] = value.astype(jnp.bfloat16)
            return carry

        lax.fori_loop(0, 4 * (cols // tile), one, 0)
        far_copy(c).start()

    def near_sum(c, r):
        def one(s, carry):
            part, value = project(c, r, 0, s)
            near[r, :, part] = (value + far_in[r, :, part].astype(jnp.float32)).astype(jnp.bfloat16)
            return carry

        lax.fori_loop(0, cols // tile, one, 0)

    def stage_f(c):
        far_copy(c).wait_recv()
        near_sum(c, 2)
        half_up_copy(c).start()
        half_down_copy(c).start()

        def three(i, carry):
            near_sum(c, i + i // 2)
            return carry

        lax.fori_loop(0, 3, three, 0)

    def add_into(r, at, other):
        near[r, :, at] = (near[r, :, at].astype(jnp.float32) + other.astype(jnp.float32)).astype(
            jnp.bfloat16
        )

    def stage_g(c):
        half_up_copy(c).wait_recv()
        add_into(1, pl.ds(c * cols, half), half_up[:, pl.ds(c * half, half)])
        full_up_copy(c).start()
        half_down_copy(c).wait_recv()
        add_into(3, pl.ds(c * cols + half, half), half_down[:, pl.ds(c * half, half)])
        full_down_copy(c).start()

    def stage_h(c):
        full_up_copy(c).wait_recv()
        full_down_copy(c).wait_recv()
        for s in range(cols // tile):
            part = pl.ds(c * cols + s * tile, tile)
            total = (
                near[0, :, part].astype(jnp.float32)
                + full_up[:, part].astype(jnp.float32)
                + full_down[:, part].astype(jnp.float32)
            ).astype(jnp.bfloat16)
            back[:, :, part] = (
                dot(spread[...], total).astype(jnp.bfloat16).reshape(n_ep, pad, tile)
            )
        start_all(back_copy, c)
        out[0, :, span_of(c)] = back[0, :, span_of(c)]

    def count_step_x():
        count_all(count_x, 3, 0, to_rows).wait_recv()
        count_y[0] = count_x[0] + count_x[1] + count_x[2] + count_x[3]
        for copy in count_copies(count_y, "grp_0", y, 1):
            copy.start()

    def count_step_y():
        count_all(count_y, 3, 1, to_up).wait_recv()
        count_e[0] = count_y[0] + count_y[1] + count_y[2] + count_y[3]

        def go(d, carry):
            remote(count_e.at[0], count_e.at[d], c_send.at[2], c_recv.at[2], ep_peer(d)).start()
            return carry

        lax.fori_loop(1, n_ep, go, 0)

    for step in range(CHUNKS + 3):
        if step < CHUNKS:
            stage_a(step)
        if step == 0:
            count_step_x()
        if 0 <= step - 1 < CHUNKS:
            stage_c(step - 1)
        if step == 1:
            count_step_y()
        if step < CHUNKS:
            stage_b(step)
        if 0 <= step - 2 < CHUNKS:
            stage_d(step - 2)
    pltpu.make_async_copy(down, w_out.at[pl.ds(0, units), :], w_local.at[2 * CHUNKS]).wait()
    down_copy.wait_recv()
    for c in range(CHUNKS):
        stage_e(c)
    for step in range(CHUNKS + 1):
        if step < CHUNKS:
            stage_f(step)
        if step >= 1:
            stage_h(step - 1)
        if step < CHUNKS:
            stage_g(step)
    count_all(count_e, n_ep - 1, 2, ep_peer(1)).wait_recv()
    totals[...] = jnp.sum(count_e[...], axis=0)
    for c in range(CHUNKS):
        z_copy(c, 1, n_ep - 1).wait_send()
        for copy in weight_copies(c):
            copy.wait_send()
        for copy in (
            swap_x(c),
            own_up(0, c),
            own_up(1, c),
            own_down(0, c),
            own_down(1, c),
            pass_up(c),
            pass_down(c),
            far_copy(c),
            half_up_copy(c),
            half_down_copy(c),
            full_up_copy(c),
            full_down_copy(c),
        ):
            copy.wait_send()
    down_copy.wait_send()
    count_all(count_x, 3, 0, to_rows).wait_send()
    count_all(count_y, 3, 1, to_up).wait_send()
    count_all(count_e, n_ep - 1, 2, ep_peer(1)).wait_send()
    for c in range(CHUNKS):
        back_copy(c, 1, n_ep - 1).wait_recv()
        back_copy(c, 1, n_ep - 1).wait_send()


def exchange(packed, counts, squeeze, spread, gate, up, down):
    n_ep, pad, width = packed.shape
    own = squeeze.shape[0]
    units = gate.shape[1]
    half = width // 2
    bf16, f32 = jnp.bfloat16, jnp.float32
    vmem = pl.BlockSpec(memory_space=pltpu.VMEM)
    hbm = pl.BlockSpec(memory_space=pl.ANY)
    dma = pltpu.SemaphoreType.DMA
    return pl.pallas_call(
        functools.partial(exchange_kernel, n_ep),
        out_shape=(
            jax.ShapeDtypeStruct((n_ep, pad, width), bf16),
            jax.ShapeDtypeStruct(counts.shape, f32),
        ),
        in_specs=[vmem, vmem, vmem, vmem, hbm, hbm, hbm],
        out_specs=(vmem, vmem),
        scratch_shapes=[
            pltpu.VMEM((n_ep, pad, width), bf16),
            pltpu.VMEM((4, 2, own, width), bf16),
            pltpu.VMEM((width, 4 * units), bf16),
            pltpu.VMEM((2 * units, width), bf16),
            pltpu.VMEM((4, 2 * own, 4 * units), f32),
            pltpu.VMEM((4, 2 * own, 2 * units), bf16),
            pltpu.VMEM((4, own, width), bf16),
            pltpu.VMEM((4, own, width), bf16),
            pltpu.VMEM((4, own, width), bf16),
            pltpu.VMEM((own, half), bf16),
            pltpu.VMEM((own, half), bf16),
            pltpu.VMEM((own, width), bf16),
            pltpu.VMEM((own, width), bf16),
            pltpu.VMEM((n_ep, pad, width), bf16),
            pltpu.VMEM((4,) + counts.shape, f32),
            pltpu.VMEM((4,) + counts.shape, f32),
            pltpu.VMEM((n_ep,) + counts.shape, f32),
            dma((CHUNKS,)),
            dma((CHUNKS,)),
            dma((CHUNKS,)),
            dma((CHUNKS,)),
            dma((12 * CHUNKS,)),
            dma((12 * CHUNKS,)),
            dma((2 * CHUNKS + 1,)),
            dma((2 * CHUNKS + 1,)),
            dma((2 * CHUNKS + 1,)),
            dma((3,)),
            dma((3,)),
        ],
        compiler_params=pltpu.CompilerParams(
            collective_id=0, has_side_effects=True, vmem_limit_bytes=67_000_000
        ),
    )(packed, counts, squeeze, spread, gate, up, down)


def body(tokens, hash_expert, gate_weight, up_weight, down_weight):
    tok_dev, model_width = tokens.shape
    ep_size = lax.axis_size(EP)
    grp_size = lax.axis_size(GRP)
    experts = gate_weight.shape[0] * ep_size
    capacity = max(2, 3 * tok_dev // (2 * experts))
    pad = -(-capacity // 16) * 16
    raw_values = tokens.astype(jnp.float32)
    normed = (
        raw_values * lax.rsqrt(jnp.mean(raw_values * raw_values, axis=-1, keepdims=True) + eps)
    ).astype(jnp.bfloat16)
    expert = hash_expert[:, 0]
    onehot = expert[:, None] == jnp.arange(experts, dtype=jnp.int32)[None, :]
    onehot_int = onehot.astype(jnp.int32)
    slot_index = jnp.sum((jnp.cumsum(onehot_int, axis=0) - 1) * onehot_int, axis=1)
    me = lax.axis_index("ep_0") * 2 + lax.axis_index("ep_1")
    target = ((expert - me + experts) % experts) * pad + slot_index
    placing = (jnp.arange(experts * pad, dtype=jnp.int32)[:, None] == target[None, :]).astype(
        jnp.bfloat16
    )
    packed = jnp.dot(placing, normed, preferred_element_type=jnp.float32).astype(jnp.bfloat16)
    packed = packed.reshape(experts, pad, model_width)
    place = jnp.arange(experts * capacity, dtype=jnp.int32)
    place = (place // capacity) * pad + place % capacity
    squeeze = place[:, None] == jnp.arange(experts * pad, dtype=jnp.int32)[None, :]
    counts = jnp.sum(onehot.astype(jnp.float32), axis=0)
    counts = jnp.pad(counts[None, :], ((0, 7), (0, 128 - experts)))
    returned, totals = exchange(
        packed,
        counts,
        squeeze.astype(jnp.bfloat16),
        squeeze.T.astype(jnp.bfloat16),
        gate_weight[0],
        up_weight[0],
        down_weight[0],
    )
    returned = returned.reshape(experts * pad, model_width)
    combined = jnp.dot(placing.T, returned, preferred_element_type=jnp.float32).astype(jnp.bfloat16)
    expert_load = totals[0, :experts] * experts / (tok_dev * grp_size * ep_size)
    balance = jnp.sum(expert_load * expert_load) / experts
    return (combined, expert_load, balance)


def solution(mesh):
    grp, ep = mesh.devices.shape
    split = Mesh(mesh.devices.reshape(4, 4, ep // 2, 2), GRP_EP)
    placed = (
        P(GRP_EP, None),
        P(GRP_EP, None),
        P(EP, None, GRP),
        P(EP, None, GRP),
        P(EP, GRP, None),
    )
    return jax.shard_map(
        body, mesh=split, in_specs=placed, out_specs=(P(GRP_EP, None), P(), P()), check_vma=False
    )
```

```python
import functools

import jax
import jax.numpy as jnp
import numpy as np
from jax import lax
from jax.experimental import pallas as pl
from jax.experimental.pallas import tpu as pltpu
from jax.sharding import Mesh
from jax.sharding import PartitionSpec as P

EP = ("ep_0", "ep_1")
GRP = ("grp_0", "grp_1")
GRP_EP = ("grp_0", "grp_1", "ep_0", "ep_1")
MESH = pl.DeviceIdType.MESH
CHUNKS = 8

eps = 1e-06


def dot(a, b):
    return jnp.dot(a, b, preferred_element_type=jnp.float32)


def exchange_kernel(
    n_ep,
    capacity,
    tokens,
    experts_of,
    squeeze,
    spread,
    gate,
    up,
    down,
    out,
    load,
    balance,
    packed,
    collect,
    returned,
    arrived,
    rows,
    w_in,
    w_out,
    acc,
    hidden,
    far,
    far_in,
    near,
    half_up,
    half_down,
    full_up,
    full_down,
    back,
    count_x,
    count_y,
    count_e,
    z_send,
    z_recv,
    b_send,
    b_recv,
    link_send,
    link_recv,
    w_send,
    w_recv,
    w_local,
    c_send,
    c_recv,
):
    pad, width = packed.shape[1], packed.shape[2]
    own = rows.shape[2]
    units = gate.shape[1]
    cols = width // CHUNKS
    half = cols // 2
    tile = min(256, cols)
    y = lax.axis_index("grp_0")
    x = lax.axis_index("grp_1")
    z = lax.axis_index("ep_0")
    core = lax.axis_index("ep_1")
    me = z * 2 + core
    flip = x + 1 - 2 * (x % 2)
    mirror = 3 - x
    row_mate = mirror + core * (flip - mirror)
    weight_mate = flip + core * (mirror - flip)
    to_rows = {"grp_1": row_mate}
    to_weights = {"grp_1": weight_mate}
    to_up = {"grp_0": (y + 1) % 4}
    to_down = {"grp_0": (y + 3) % 4}

    def ep_peer(d):
        t = (me + d) % n_ep
        return {"ep_0": t // 2, "ep_1": t % 2}

    barrier = pltpu.get_barrier_semaphore()

    def greet(d, carry):
        pl.semaphore_signal(barrier, inc=1, device_id=ep_peer(d), device_id_type=MESH)
        return carry

    lax.fori_loop(1, n_ep, greet, 0)
    for j in range(1, 4):
        pl.semaphore_signal(barrier, inc=1, device_id={"grp_1": (x + j) % 4}, device_id_type=MESH)
        pl.semaphore_signal(barrier, inc=1, device_id={"grp_0": (y + j) % 4}, device_id_type=MESH)
    for r in range(2):
        for c in range(CHUNKS):
            span = pl.ds(c * cols, cols)
            pltpu.make_async_copy(
                (gate, up)[r].at[span, :],
                w_in.at[span, pl.ds(r * units, units)],
                w_local.at[r * CHUNKS + c],
            ).start()
    pltpu.make_async_copy(down, w_out.at[pl.ds(0, units), :], w_local.at[2 * CHUNKS]).start()

    n_tok = tokens.shape[0]
    f32, bf16 = jnp.float32, jnp.bfloat16
    named = experts_of[...]
    picks = (lax.broadcasted_iota(jnp.int32, (n_ep, n_tok), 0) == named).astype(f32)
    before = lax.broadcasted_iota(jnp.int32, (n_tok, n_tok), 0) < lax.broadcasted_iota(
        jnp.int32, (n_tok, n_tok), 1
    )
    earlier = dot(picks.astype(bf16), before.astype(bf16))
    slot = jnp.sum(earlier * picks, axis=0, keepdims=True).astype(jnp.int32)
    away = named - me
    away = jnp.where(away < 0, away + n_ep, away)
    target = away * pad + slot
    placing = (
        lax.broadcasted_iota(jnp.int32, (n_ep * pad, n_tok), 0) == target
    ).astype(f32).astype(bf16)
    same = lax.broadcasted_iota(jnp.int32, (n_tok, n_tok), 0) == lax.broadcasted_iota(
        jnp.int32, (n_tok, n_tok), 1
    )
    target_down = jnp.sum(jnp.where(same, target.astype(f32), 0.0), axis=1, keepdims=True).astype(
        jnp.int32
    )
    collect[...] = (
        lax.broadcasted_iota(jnp.int32, (n_tok, n_ep * pad), 1) == target_down
    ).astype(f32).astype(bf16)
    count_x[0] = jnp.broadcast_to(jnp.sum(picks, axis=1, keepdims=True), count_x.shape[1:])
    step = min(512, width)
    squares = jnp.zeros((n_tok, 1), f32)
    for s in range(width // step):
        value = tokens[:, pl.ds(s * step, step)].astype(f32)
        squares += jnp.sum(value * value, axis=1, keepdims=True)
    scale = lax.rsqrt(squares / width + eps)
    for s in range(width // step):
        part = pl.ds(s * step, step)
        normed = (tokens[:, part].astype(f32) * scale).astype(bf16)
        packed[:, :, part] = dot(placing, normed).astype(bf16).reshape(n_ep, pad, step)
    arrived[0] = packed[0]
    pl.semaphore_wait(barrier, n_ep - 1 + 6)

    def remote(src, dst, send, recv, device):
        return pltpu.make_async_remote_copy(
            src_ref=src,
            dst_ref=dst,
            send_sem=send,
            recv_sem=recv,
            device_id=device,
            device_id_type=MESH,
        )

    def span_of(c):
        return pl.ds(c * cols, cols)

    def z_copy(c, d, n=None):
        at = d if n is None else pl.ds(d, n)
        return remote(
            packed.at[at, :, span_of(c)],
            arrived.at[at, :, span_of(c)],
            z_send.at[c],
            z_recv.at[c],
            ep_peer(d),
        )

    def back_copy(c, d, n=None):
        at = d if n is None else pl.ds(d, n)
        return remote(
            back.at[at, :, span_of(c)],
            returned.at[at, :, span_of(c)],
            b_send.at[c],
            b_recv.at[c],
            ep_peer(n_ep - d),
        )

    def start_all(copy_of, c):
        def go(d, carry):
            copy_of(c, d).start()
            return carry

        lax.fori_loop(1, n_ep, go, 0)

    def weight_copies(c):
        return [
            remote(
                (gate, up)[r].at[span_of(c), :],
                w_in.at[span_of(c), pl.ds((2 + r) * units, units)],
                w_send.at[r * CHUNKS + c],
                w_recv.at[r * CHUNKS + c],
                to_weights,
            )
            for r in range(2)
        ]

    def down_copy(c):
        return remote(
            down.at[:, span_of(c)],
            w_out.at[pl.ds(units, units), span_of(c)],
            w_send.at[2 * CHUNKS + c],
            w_recv.at[2 * CHUNKS + c],
            to_weights,
        )

    def count_copies(buffer, axis, at, sem):
        return [
            remote(buffer.at[0], buffer.at[j], c_send.at[sem], c_recv.at[sem], {axis: (at + j) % 4})
            for j in range(1, 4)
        ]

    def count_all(buffer, n, sem, device):
        return remote(
            buffer.at[pl.ds(1, n)], buffer.at[pl.ds(1, n)], c_send.at[sem], c_recv.at[sem], device
        )

    for copy in count_copies(count_x, "grp_1", x, 0):
        copy.start()

    def link(kind, c, src, dst, device):
        return remote(
            src, dst, link_send.at[kind * CHUNKS + c], link_recv.at[kind * CHUNKS + c], device
        )

    def block(r, k, c):
        return rows.at[r, k, :, span_of(c)]

    def swap_x(c):
        return link(0, c, block(0, 0, c), block(0, 1, c), to_rows)

    def own_up(k, c):
        return link(1 + k, c, block(0, k, c), block(3, k, c), to_up)

    def own_down(k, c):
        return link(3 + k, c, block(0, k, c), block(1, k, c), to_down)

    def pass_up(c):
        return link(5, c, block(3, 0, c), block(2, 0, c), to_up)

    def pass_down(c):
        return link(6, c, block(1, 1, c), block(2, 1, c), to_down)

    def far_copy(c):
        return link(7, c, far.at[:, :, span_of(c)], far_in.at[:, :, span_of(c)], to_rows)

    def half_up_copy(c):
        return link(
            8,
            c,
            near.at[2, :, pl.ds(c * cols, half)],
            half_up.at[:, pl.ds(c * half, half)],
            to_up,
        )

    def half_down_copy(c):
        return link(
            9,
            c,
            near.at[2, :, pl.ds(c * cols + half, half)],
            half_down.at[:, pl.ds(c * half, half)],
            to_down,
        )

    def full_up_copy(c):
        return link(10, c, near.at[1, :, span_of(c)], full_up.at[:, span_of(c)], to_up)

    def full_down_copy(c):
        return link(11, c, near.at[3, :, span_of(c)], full_down.at[:, span_of(c)], to_down)

    def stage_a(c):
        z_copy(c, 1, n_ep - 1).wait_recv()
        span = span_of(c)
        step = min(512, cols)
        for s in range(cols // step):
            part = pl.ds(c * cols + s * step, step)
            rows[0, 0, :, part] = dot(
                squeeze[...], arrived[:, :, part].reshape(n_ep * pad, step)
            ).astype(jnp.bfloat16)
        swap_x(c).start()
        own_up(0, c).start()
        own_down(0, c).start()

    def stage_b(c):
        swap_x(c).wait_recv()
        own_up(1, c).start()
        own_down(1, c).start()

    def stage_c(c):
        own_up(0, c).wait_recv()
        pass_up(c).start()
        own_down(1, c).wait_recv()
        pass_down(c).start()

    def multiply(c, r):
        left = rows[r, :, :, span_of(c)].reshape(2 * own, cols)

        def one(n, carry):
            part = pl.ds(pl.multiple_of(n * units, units), units)
            product = dot(left, w_in[span_of(c), part])
            if c == 0:
                acc[r, :, part] = product
            else:
                acc[r, :, part] += product
            return carry

        lax.fori_loop(0, 4, one, 0)
        if c == CHUNKS - 1:
            for k in range(2):
                g = acc[r, :, pl.ds(2 * k * units, units)]
                u = acc[r, :, pl.ds((2 * k + 1) * units, units)]
                hidden[r, :, pl.ds(k * units, units)] = (jax.nn.silu(g) * u).astype(jnp.bfloat16)

    def stage_d(c):
        for r in range(2):
            pltpu.make_async_copy(
                (gate, up)[r].at[span_of(c), :],
                w_in.at[span_of(c), pl.ds(r * units, units)],
                w_local.at[r * CHUNKS + c],
            ).wait()
        for copy in weight_copies(c):
            copy.wait_recv()
        own_down(0, c).wait_recv()
        own_up(1, c).wait_recv()

        def three(i, carry):
            multiply(c, i + i // 2)
            return carry

        lax.fori_loop(0, 3, three, 0)
        pass_up(c).wait_recv()
        pass_down(c).wait_recv()
        multiply(c, 2)

    def project(c, r, k, s):
        part = pl.ds(pl.multiple_of(c * cols + s * tile, tile), tile)
        return part, dot(hidden[r, pl.ds(k * own, own), :], w_out[:, part])

    def stage_e(c):
        def one(i, carry):
            r, s = i // (cols // tile), i % (cols // tile)
            part, value = project(c, r, 1, s)
            far[r, :, part] = value.astype(jnp.bfloat16)
            return carry

        lax.fori_loop(0, 4 * (cols // tile), one, 0)
        far_copy(c).start()

    def near_sum(c, r):
        def one(s, carry):
            part, value = project(c, r, 0, s)
            near[r, :, part] = (value + far_in[r, :, part].astype(jnp.float32)).astype(jnp.bfloat16)
            return carry

        lax.fori_loop(0, cols // tile, one, 0)

    def stage_f(c):
        far_copy(c).wait_recv()
        near_sum(c, 2)
        half_up_copy(c).start()
        half_down_copy(c).start()

        def three(i, carry):
            near_sum(c, i + i // 2)
            return carry

        lax.fori_loop(0, 3, three, 0)

    def add_into(r, at, other):
        near[r, :, at] = (near[r, :, at].astype(jnp.float32) + other.astype(jnp.float32)).astype(
            jnp.bfloat16
        )

    def stage_g(c):
        half_up_copy(c).wait_recv()
        add_into(1, pl.ds(c * cols, half), half_up[:, pl.ds(c * half, half)])
        full_up_copy(c).start()
        half_down_copy(c).wait_recv()
        add_into(3, pl.ds(c * cols + half, half), half_down[:, pl.ds(c * half, half)])
        full_down_copy(c).start()

    def stage_h(c):
        full_up_copy(c).wait_recv()
        full_down_copy(c).wait_recv()
        for s in range(cols // tile):
            part = pl.ds(c * cols + s * tile, tile)
            total = (
                near[0, :, part].astype(jnp.float32)
                + full_up[:, part].astype(jnp.float32)
                + full_down[:, part].astype(jnp.float32)
            ).astype(jnp.bfloat16)
            back[:, :, part] = (
                dot(spread[...], total).astype(jnp.bfloat16).reshape(n_ep, pad, tile)
            )
        start_all(back_copy, c)
        returned[0, :, span_of(c)] = back[0, :, span_of(c)]

    def stage_i(c):
        back_copy(c, 1, n_ep - 1).wait_recv()
        block_rows = returned[:, :, span_of(c)].reshape(n_ep * pad, cols)
        out[:, span_of(c)] = dot(collect[...], block_rows).astype(bf16)

    def count_step_x():
        count_all(count_x, 3, 0, to_rows).wait_recv()
        count_y[0] = count_x[0] + count_x[1] + count_x[2] + count_x[3]
        for copy in count_copies(count_y, "grp_0", y, 1):
            copy.start()

    def count_step_y():
        count_all(count_y, 3, 1, to_up).wait_recv()
        count_e[0] = count_y[0] + count_y[1] + count_y[2] + count_y[3]

        def go(d, carry):
            remote(count_e.at[0], count_e.at[d], c_send.at[2], c_recv.at[2], ep_peer(d)).start()
            return carry

        lax.fori_loop(1, n_ep, go, 0)

    start_all(z_copy, 0)
    for copy in weight_copies(0):
        copy.start()
    start_all(z_copy, 1)
    for step in range(CHUNKS + 2):
        if step < CHUNKS:
            stage_a(step)
        if step + 2 < CHUNKS:
            start_all(z_copy, step + 2)
        if step == 0:
            count_step_x()
        if 0 <= step - 1 < CHUNKS:
            stage_c(step - 1)
        if step == 1:
            count_step_y()
        if step < CHUNKS:
            stage_b(step)
        if step + 1 < CHUNKS:
            for copy in weight_copies(step + 1):
                copy.start()
        if step < CHUNKS:
            down_copy(step).start()
        if 0 <= step - 2 < CHUNKS:
            stage_d(step - 2)
    pltpu.make_async_copy(down, w_out.at[pl.ds(0, units), :], w_local.at[2 * CHUNKS]).wait()
    for c in range(CHUNKS):
        down_copy(c).wait_recv()
    stage_e(0)
    stage_e(1)
    for step in range(CHUNKS + 3):
        if step < CHUNKS:
            stage_f(step)
        if step + 2 < CHUNKS:
            stage_e(step + 2)
        if 1 <= step <= CHUNKS:
            stage_h(step - 1)
        if step < CHUNKS:
            stage_g(step)
        if step >= 3:
            stage_i(step - 3)
    count_all(count_e, n_ep - 1, 2, ep_peer(1)).wait_recv()
    share = jnp.sum(count_e[...], axis=0) * n_ep / (n_tok * 16 * n_ep)
    at_lane = lax.broadcasted_iota(jnp.int32, share.shape, 0) == lax.broadcasted_iota(
        jnp.int32, share.shape, 1
    )
    load[...] = jnp.sum(jnp.where(at_lane, share, 0.0), axis=0, keepdims=True)
    balance[...] = jnp.sum(share * share, axis=0, keepdims=True) / n_ep
    for c in range(CHUNKS):
        z_copy(c, 1, n_ep - 1).wait_send()
        for copy in weight_copies(c):
            copy.wait_send()
        down_copy(c).wait_send()
        for copy in (
            swap_x(c),
            own_up(0, c),
            own_up(1, c),
            own_down(0, c),
            own_down(1, c),
            pass_up(c),
            pass_down(c),
            far_copy(c),
            half_up_copy(c),
            half_down_copy(c),
            full_up_copy(c),
            full_down_copy(c),
        ):
            copy.wait_send()
    count_all(count_x, 3, 0, to_rows).wait_send()
    count_all(count_y, 3, 1, to_up).wait_send()
    count_all(count_e, n_ep - 1, 2, ep_peer(1)).wait_send()
    for c in range(CHUNKS):
        back_copy(c, 1, n_ep - 1).wait_send()


def body(tokens, hash_expert, gate_weight, up_weight, down_weight):
    n_tok, width = tokens.shape
    n_ep = lax.axis_size(EP)
    units = gate_weight.shape[2]
    capacity = max(2, 3 * n_tok // (2 * n_ep))
    pad = -(-capacity // 16) * 16
    own = n_ep * capacity
    half = width // 2
    place = np.arange(own)
    place = (place // capacity) * pad + place % capacity
    squeeze = place[:, None] == np.arange(n_ep * pad)[None, :]
    bf16, f32 = jnp.bfloat16, jnp.float32
    vmem = pl.BlockSpec(memory_space=pltpu.VMEM)
    hbm = pl.BlockSpec(memory_space=pl.ANY)
    dma = pltpu.SemaphoreType.DMA
    combined, load, balance = pl.pallas_call(
        functools.partial(exchange_kernel, n_ep, capacity),
        out_shape=(
            jax.ShapeDtypeStruct((n_tok, width), bf16),
            jax.ShapeDtypeStruct((1, 128), f32),
            jax.ShapeDtypeStruct((1, 128), f32),
        ),
        in_specs=[vmem, vmem, vmem, vmem, hbm, hbm, hbm],
        out_specs=(vmem, vmem, vmem),
        scratch_shapes=[
            pltpu.VMEM((n_ep, pad, width), bf16),
            pltpu.VMEM((n_tok, n_ep * pad), bf16),
            pltpu.VMEM((n_ep, pad, width), bf16),
            pltpu.VMEM((n_ep, pad, width), bf16),
            pltpu.VMEM((4, 2, own, width), bf16),
            pltpu.VMEM((width, 4 * units), bf16),
            pltpu.VMEM((2 * units, width), bf16),
            pltpu.VMEM((4, 2 * own, 4 * units), f32),
            pltpu.VMEM((4, 2 * own, 2 * units), bf16),
            pltpu.VMEM((4, own, width), bf16),
            pltpu.VMEM((4, own, width), bf16),
            pltpu.VMEM((4, own, width), bf16),
            pltpu.VMEM((own, half), bf16),
            pltpu.VMEM((own, half), bf16),
            pltpu.VMEM((own, width), bf16),
            pltpu.VMEM((own, width), bf16),
            pltpu.VMEM((n_ep, pad, width), bf16),
            pltpu.VMEM((4, n_ep, 128), f32),
            pltpu.VMEM((4, n_ep, 128), f32),
            pltpu.VMEM((n_ep, n_ep, 128), f32),
            dma((CHUNKS,)),
            dma((CHUNKS,)),
            dma((CHUNKS,)),
            dma((CHUNKS,)),
            dma((12 * CHUNKS,)),
            dma((12 * CHUNKS,)),
            dma((3 * CHUNKS,)),
            dma((3 * CHUNKS,)),
            dma((2 * CHUNKS + 1,)),
            dma((3,)),
            dma((3,)),
        ],
        compiler_params=pltpu.CompilerParams(
            collective_id=0, has_side_effects=True, vmem_limit_bytes=67_000_000
        ),
    )(
        tokens,
        hash_expert.reshape(1, n_tok),
        jnp.asarray(squeeze, dtype=bf16),
        jnp.asarray(squeeze.T, dtype=bf16),
        gate_weight[0],
        up_weight[0],
        down_weight[0],
    )
    return (combined, load[0, :n_ep], balance[0, 0])


def solution(mesh):
    grp, ep = mesh.devices.shape
    split = Mesh(mesh.devices.reshape(4, 4, ep // 2, 2), GRP_EP)
    placed = (
        P(GRP_EP, None),
        P(GRP_EP, None),
        P(EP, None, GRP),
        P(EP, None, GRP),
        P(EP, GRP, None),
    )
    return jax.shard_map(
        body, mesh=split, in_specs=placed, out_specs=(P(GRP_EP, None), P(), P()), check_vma=False
    )
```
